32 devices in a mesh: row: 4 (over y, core), col: 8 (over z, x).
Axes of the slice: x: 2, y: 2, z: 4, core: 2. Of those that a mesh axis runs over, the one named last changes fastest.
Arguments:
- phase: float32 [512, 32, 512], P('col', 'row'), may hold values from -6 to 6
- velocity: float32 [3, 512, 32, 512], P(None, 'col', 'row'), may hold values from -12 to 12
Outputs:
- phase_next: float32 [512, 32, 512], P('col', 'row')
- velocity_next: float32 [3, 512, 32, 512], P(None, 'col', 'row')
The draws below stay inside these ranges and needn't reach their ends.
All inputs are finite; a program needn't handle non-finite values.
Results may differ from the reference program's by a relative error of at most 0.013.
Values may be sent and summed in bfloat16 or wider, within the bound.
A program may use at most 128 MiB of HBM per device.

```python
import math
import jax
import jax.numpy as jnp
from jax import lax

NX = 512
NY = 512
NZ = 32
KC = 192
KY = 384
KZH = 12
KZ = 24


def block_scale(rng, shape, cuts, low, largest):
    def one(dim, parts):
        heights = jax.random.uniform(jax.random.fold_in(jax.random.fold_in(rng, 6), dim), (parts,), jnp.float32, low / len(cuts), largest / len(cuts))
        return jnp.repeat(jnp.exp(heights), shape[dim] // parts).reshape((-1,) + (1,) * (len(shape) - dim - 1))

    factor_of = one(*cuts[0])
    for cut in cuts[1:]:
        factor_of = factor_of * one(*cut)
    return factor_of


def gaussian(key, extent, scale, reach, split=(), kind=jnp.bfloat16):
    gain = block_scale(key, extent, split, -0.22, 0.18) if split else 1.0
    drawn = jax.random.normal(key, extent, jnp.float32) * scale * gain
    return jnp.minimum(jnp.maximum(drawn, -reach), reach).astype(kind)


def setup_inputs(seed: int = 0) -> dict:
    key_of = jax.random.split(jax.random.key(seed), 3)
    return {
        "phase": gaussian(key_of[0], (NY, NZ, NX), 1.0, 6.0, ((0, 8), (1, 4)), jnp.float32),
        "velocity": gaussian(key_of[1], (3, NY, NZ, NX), 2.0, 12.0, ((1, 8), (2, 4)), jnp.float32),
    }


time_step = 1e-3
epsilon = 0.01
mobility = 1.0
reynolds = 100.0
stabilizer = 2.0


def cos_sin(row_index, col_index, period):
    residue = (row_index[:, None] * col_index[None, :]) % period
    angles = residue.astype(jnp.float32) * (2.0 * math.pi / period)
    return jnp.stack([jnp.cos(angles), jnp.sin(angles)]).astype(jnp.bfloat16)


def pair_sum(pieces, direction, stack_axis):
    if direction < 0:
        real_part = pieces[0, 0] + pieces[1, 1]
        imag_part = pieces[1, 0] - pieces[0, 1]
    else:
        real_part = pieces[0, 0] - pieces[1, 1]
        imag_part = pieces[0, 1] + pieces[1, 0]
    return jnp.stack([real_part, imag_part], axis=stack_axis)


def rounded(values):
    return lax.optimization_barrier(values.astype(jnp.bfloat16))


def product(form, first_op, second_op):
    return jnp.einsum(form, first_op.astype(jnp.float32), second_op.astype(jnp.float32), precision=lax.Precision.HIGHEST)


def times_i(values):
    return jnp.stack([-values[1], values[0]])


def reference(phase, velocity):
    table_x = cos_sin(jnp.arange(NX, dtype=jnp.int32), jnp.arange(KC, dtype=jnp.int32), NX)
    table_y = cos_sin(jnp.arange(NY, dtype=jnp.int32), jnp.arange(KY, dtype=jnp.int32) - KC, NY)
    table_z = cos_sin(jnp.arange(NZ, dtype=jnp.int32), jnp.arange(KZ, dtype=jnp.int32) - KZH, NZ)
    scale_inv = 1.0 / (NX * NY * NZ)
    weight = jnp.where(jnp.arange(KC) == 0, 1.0, 2.0).astype(jnp.float32)[:, None, None]

    def forward(field):
        pieces = product('yzx,txa->tayz', rounded(field), table_x)
        x_lines = rounded(jnp.stack([pieces[0], -pieces[1]]))
        pieces = product('payz,tyb->ptabz', x_lines, table_y)
        y_planes = rounded(pair_sum(pieces, -1, 0))
        pieces = product('pabz,tzm->ptabm', y_planes, table_z)
        return pair_sum(pieces, -1, 0) * scale_inv

    def inverse(coeff):
        pieces = product('pabm,tzm->ptabz', rounded(coeff), table_z)
        z_planes = rounded(pair_sum(pieces, 1, 0))
        pieces = product('pabz,tyb->ptayz', z_planes, table_y)
        x_lines = rounded(pair_sum(pieces, 1, 0))
        scaled = jnp.stack([x_lines[0] * weight, -(x_lines[1] * weight)])
        return product('payz,pxa->yzx', scaled, table_x)

    wave_x = jnp.arange(KC).astype(jnp.float32)[None, :, None, None]
    wave_y = (jnp.arange(KY) - KC).astype(jnp.float32)[None, None, :, None]
    wave_z = ((jnp.arange(KZ) - KZH).astype(jnp.float32) * (NX / NZ))[None, None, None, :]
    squared = wave_x * wave_x + wave_y * wave_y + wave_z * wave_z

    coeff_phase = forward(phase)
    coeff_u = [forward(velocity[j]) for j in range(3)]
    gradient = [inverse(times_i(wave_x * coeff_phase)), inverse(times_i(wave_y * coeff_phase)), inverse(times_i(wave_z * coeff_phase))]
    lap_field = inverse(-squared * coeff_phase)
    vortex = [inverse(times_i(wave_y * coeff_u[2] - wave_z * coeff_u[1])),
              inverse(times_i(wave_z * coeff_u[0] - wave_x * coeff_u[2])),
              inverse(times_i(wave_x * coeff_u[1] - wave_y * coeff_u[0]))]
    advect = velocity[0] * gradient[0] + velocity[1] * gradient[1] + velocity[2] * gradient[2]
    bulk_term = phase * phase * phase - phase
    potential = bulk_term - epsilon * epsilon * lap_field
    forcing = [velocity[1] * vortex[2] - velocity[2] * vortex[1] + potential * gradient[0],
               velocity[2] * vortex[0] - velocity[0] * vortex[2] + potential * gradient[1],
               velocity[0] * vortex[1] - velocity[1] * vortex[0] + potential * gradient[2]]
    mean_mode = (wave_x == 0) & (wave_y == 0) & (wave_z == 0)
    advect_hat = jnp.where(mean_mode, 0.0, forward(advect))
    bulk_hat = forward(bulk_term)
    force_hat = [forward(forcing[j]) for j in range(3)]
    stable_part = 1.0 / time_step + mobility * stabilizer * squared
    new_phase = (stable_part * coeff_phase - advect_hat - mobility * squared * bulk_hat) / (stable_part + mobility * epsilon * epsilon * squared * squared)
    viscous = 1.0 / time_step + squared / reynolds
    unprojected = [(coeff_u[j] / time_step + force_hat[j]) / viscous for j in range(3)]
    normal_part = (wave_x * unprojected[0] + wave_y * unprojected[1] + wave_z * unprojected[2]) / jnp.maximum(squared, 1.0)
    waves = [wave_x, wave_y, wave_z]
    phase_next = inverse(new_phase)
    velocity_next = jnp.stack([inverse(unprojected[j] - waves[j] * normal_part) for j in range(3)])
    return phase_next, velocity_next
```

```python
import math

import jax
import jax.numpy as jnp
import ml_dtypes
import numpy as np
from jax import lax
from jax.experimental import pallas as pl
from jax.experimental.pallas import tpu as pltpu
from jax.sharding import PartitionSpec as P

NX = 512
NY = 512
KC = 192
KY = 384


time_step = 0.001
epsilon = 0.01
mobility = 1.0
reynolds = 100.0
stabilizer = 2.0


def cos_sin(row_index, col_index, period):
    residue = row_index[:, None] * col_index[None, :] % period
    angles = residue.astype(jnp.float32) * (2.0 * math.pi / period)
    return jnp.stack([jnp.cos(angles), jnp.sin(angles)]).astype(jnp.bfloat16)


def pair_sum(pieces, direction, stack_axis):
    if direction < 0:
        real_part = pieces[0, 0] + pieces[1, 1]
        imag_part = pieces[1, 0] - pieces[0, 1]
    else:
        real_part = pieces[0, 0] - pieces[1, 1]
        imag_part = pieces[0, 1] + pieces[1, 0]
    return jnp.stack([real_part, imag_part], axis=stack_axis)


def times_i(values):
    return jnp.stack([-values[:, 1], values[:, 0]], axis=1)


def phase_terms(phase, velocity, gradient, lap_field):
    advect = velocity[0] * gradient[0] + velocity[1] * gradient[1] + velocity[2] * gradient[2]
    bulk_term = phase * phase * phase - phase
    potential = bulk_term - epsilon * epsilon * lap_field
    return (advect, bulk_term, potential)


def momentum(velocity, vortex, gradient, potential):
    return jnp.stack(
        [
            velocity[1] * vortex[2] - velocity[2] * vortex[1] + potential * gradient[0],
            velocity[2] * vortex[0] - velocity[0] * vortex[2] + potential * gradient[1],
            velocity[0] * vortex[1] - velocity[1] * vortex[0] + potential * gradient[2],
        ]
    )


def plain_device(phase, velocity):
    col_count = lax.axis_size("col")
    row_count = lax.axis_size("row")
    rows_y = phase.shape[0]
    planes = phase.shape[1]
    total_z = planes * row_count
    half_z = 3 * total_z // 8
    modes_z = 2 * half_z
    kx_local = KC // col_count
    ky_local = KY // row_count
    scale_inv = 1.0 / (NX * NY * total_z)
    table_x = cos_sin(jnp.arange(NX, dtype=jnp.int32), jnp.arange(KC, dtype=jnp.int32), NX)
    table_y = cos_sin(jnp.arange(NY, dtype=jnp.int32), jnp.arange(KY, dtype=jnp.int32) - KC, NY)
    table_z = cos_sin(
        jnp.arange(total_z, dtype=jnp.int32), jnp.arange(modes_z, dtype=jnp.int32) - half_z, total_z
    )
    y_forward = table_y.reshape(2, col_count, rows_y, KY)
    y_inverse = table_y.reshape(2, col_count, rows_y, row_count, ky_local)
    z_table = table_z.reshape(2, row_count, planes, modes_z)
    weight = jnp.where(jnp.arange(KC) == 0, 1.0, 2.0).astype(jnp.bfloat16)[:, None, None, None]

    def along_y(incoming):
        field_count = incoming.shape[1]
        shaped = incoming.reshape(incoming.shape[0], field_count, col_count, 2, rows_y, planes)
        pieces = jnp.einsum(
            "afcpyz,tcyb->ptafbz", shaped, y_forward, preferred_element_type=jnp.float32
        )
        joined = pair_sum(pieces, -1, 2).astype(jnp.bfloat16)
        return joined.reshape(incoming.shape[0], field_count, 2, KY * planes)

    def along_z(incoming):
        field_count = incoming.shape[1]
        shaped = incoming.reshape(incoming.shape[0], field_count, 2, row_count, ky_local, planes)
        pieces = jnp.einsum(
            "afprbz,trzm->ptafbm", shaped, z_table, preferred_element_type=jnp.float32
        )
        joined = pair_sum(pieces, -1, 2) * scale_inv
        return joined.reshape(incoming.shape[0], field_count, 2, ky_local * modes_z)

    def back_y(incoming):
        field_count = incoming.shape[1]
        shaped = incoming.reshape(incoming.shape[0], field_count, 2, row_count, planes, ky_local)
        pieces = jnp.einsum(
            "afprzb,tcyrb->ptafcyz", shaped, y_inverse, preferred_element_type=jnp.float32
        )
        joined = pair_sum(pieces, 1, 3).astype(jnp.bfloat16)
        return joined.reshape(incoming.shape[0], field_count, col_count * 2 * rows_y * planes)

    def back_x(incoming):
        field_count = incoming.shape[1]
        shaped = incoming.reshape(KC, field_count, 2, rows_y, planes)
        scaled = jnp.stack([shaped[:, :, 0] * weight, -(shaped[:, :, 1] * weight)], axis=2)
        return jnp.einsum("afpyz,pxa->fyzx", scaled, table_x, preferred_element_type=jnp.float32)

    def forward(fields):
        field_count = fields.shape[0]
        pieces = jnp.einsum(
            "fyzx,txa->tafyz",
            fields.astype(jnp.bfloat16),
            table_x,
            preferred_element_type=jnp.float32,
        )
        x_lines = jnp.stack([pieces[0], -pieces[1]], axis=2).astype(jnp.bfloat16)
        x_lines = x_lines.reshape(KC, field_count, 2 * rows_y * planes)
        spread = along_y(lax.all_to_all(x_lines, "col", split_axis=0, concat_axis=2, tiled=True))
        return along_z(lax.all_to_all(spread, "row", split_axis=3, concat_axis=3, tiled=True))

    def inverse(spectra):
        field_count = spectra.shape[1]
        shaped = spectra.astype(jnp.bfloat16).reshape(kx_local, field_count, 2, ky_local, modes_z)
        pieces = jnp.einsum(
            "afpbm,trzm->ptafrzb", shaped, z_table, preferred_element_type=jnp.float32
        )
        z_planes = (
            pair_sum(pieces, 1, 2)
            .astype(jnp.bfloat16)
            .reshape(kx_local, field_count, 2, total_z * ky_local)
        )
        spread = back_y(lax.all_to_all(z_planes, "row", split_axis=3, concat_axis=3, tiled=True))
        return back_x(lax.all_to_all(spread, "col", split_axis=2, concat_axis=0, tiled=True))

    spectra = forward(jnp.concatenate([phase[None], velocity], axis=0))
    wave_x = (lax.axis_index("col") * kx_local + jnp.arange(kx_local, dtype=jnp.int32)).astype(
        jnp.float32
    )[:, None, None]
    modes_y = lax.axis_index("row") * ky_local + jnp.arange(ky_local, dtype=jnp.int32) - KC
    wave_y = jnp.broadcast_to(modes_y.astype(jnp.float32)[:, None], (ky_local, modes_z)).reshape(-1)
    z_values = (jnp.arange(modes_z, dtype=jnp.int32) - half_z).astype(jnp.float32) * (NX / total_z)
    wave_z = jnp.broadcast_to(z_values[None, :], (ky_local, modes_z)).reshape(-1)
    squared = wave_x * wave_x + wave_y * wave_y + wave_z * wave_z
    coeff_phase = spectra[:, 0]
    coeff_u = spectra[:, 1]
    coeff_v = spectra[:, 2]
    coeff_w = spectra[:, 3]
    gradients = [
        times_i(wave_x * coeff_phase),
        times_i(wave_y * coeff_phase),
        times_i(wave_z * coeff_phase),
    ]
    laplace = -squared * coeff_phase
    vortex_hat = [
        times_i(wave_y * coeff_w - wave_z * coeff_v),
        times_i(wave_z * coeff_u - wave_x * coeff_w),
        times_i(wave_x * coeff_v - wave_y * coeff_u),
    ]
    leading = inverse(jnp.stack(gradients + [laplace], axis=1))
    advect, bulk_term, potential = phase_terms(phase, velocity, leading[0:3], leading[3])
    phase_side = forward(jnp.stack([advect, bulk_term]))
    vortex = inverse(jnp.stack(vortex_hat, axis=1))
    flow_side = forward(momentum(velocity, vortex, leading[0:3], potential))
    nonlinear = jnp.concatenate([phase_side, flow_side], axis=1)
    mean_mode = (wave_x == 0) & (wave_y == 0) & (wave_z == 0)
    advect_hat = jnp.where(mean_mode, 0.0, nonlinear[:, 0])
    bulk_hat = nonlinear[:, 1]
    stable_part = 1.0 / time_step + mobility * stabilizer * squared
    new_phase = (stable_part * coeff_phase - advect_hat - mobility * squared * bulk_hat) / (
        stable_part + mobility * epsilon * epsilon * squared * squared
    )
    viscous = 1.0 / time_step + squared / reynolds
    unprojected = [
        (spectra[:, 1 + j] / time_step + nonlinear[:, 2 + j]) / viscous for j in range(3)
    ]
    normal_part = (
        wave_x * unprojected[0] + wave_y * unprojected[1] + wave_z * unprojected[2]
    ) / jnp.maximum(squared, 1.0)
    waves = [wave_x, wave_y, wave_z]
    new_flow = [unprojected[j] - waves[j] * normal_part for j in range(3)]
    result = inverse(jnp.stack([new_phase] + new_flow, axis=1))
    return (result[0], result[1:4])


def tables(cols, rows, rows_y, planes):
    total_z = planes * rows
    half_z = 3 * total_z // 8
    modes_z = 2 * half_z
    kx_local = KC // cols

    def pair(first, second, period):
        residue = first[:, None] * second[None, :] % period
        angles = residue.astype(np.float32) * np.float32(2.0 * math.pi / period)
        return [np.cos(angles).astype(ml_dtypes.bfloat16), np.sin(angles).astype(ml_dtypes.bfloat16)]

    cos_x, sin_x = pair(np.arange(KC), np.arange(NX), NX)
    cos_y, sin_y = pair(np.arange(NY), np.arange(KY) - KC, NY)
    cos_z, sin_z = pair(np.arange(total_z), np.arange(modes_z) - half_z, total_z)
    x_forward = np.stack([cos_x, -sin_x]).reshape(2, cols, kx_local, NX)
    x_forward = x_forward.transpose(1, 0, 2, 3).reshape(2 * KC, NX)
    weight = np.where(np.arange(KC) == 0, 1.0, 2.0).astype(ml_dtypes.bfloat16)[:, None]
    x_inverse = np.stack([cos_x * weight, -(sin_x * weight)]).reshape(2, cols, kx_local, NX)
    x_inverse = x_inverse.transpose(1, 0, 2, 3).reshape(2 * KC, NX)
    y_forward = np.concatenate([cos_y, sin_y], axis=1)
    y_inverse = np.concatenate([cos_y.T, sin_y.T], axis=1)
    cz, sz = (t.reshape(rows, planes, modes_z) for t in (cos_z, sin_z))
    z_forward = np.stack([np.stack([cz, sz], 1), np.stack([-sz, cz], 1)])
    z_forward = z_forward.transpose(0, 4, 1, 2, 3).reshape(2 * modes_z, 2 * total_z)
    z_inverse = np.stack([np.stack([cz, -sz], 2), np.stack([sz, cz], 2)], 1)
    z_inverse = z_inverse.reshape(2 * total_z, 2 * modes_z)
    return [jnp.asarray(t.astype(ml_dtypes.bfloat16)) for t in (x_forward, x_inverse, y_forward, y_inverse, z_forward, z_inverse)]


def dot(first, second, dims=((1,), (0,))):
    return lax.dot_general(first, second, (dims, ((), ())), preferred_element_type=jnp.float32)


def whole(array):
    return pl.BlockSpec(array.shape, lambda *_: (0,) * array.ndim)


def call(body, grid, in_specs, out_specs, out_shape, flops, moved, scratch=()):
    return pl.pallas_call(
        body,
        grid=grid,
        in_specs=in_specs,
        out_specs=out_specs,
        out_shape=out_shape,
        scratch_shapes=list(scratch),
        compiler_params=pltpu.CompilerParams(vmem_limit_bytes=40 * 1024 * 1024),
        cost_estimate=pl.CostEstimate(flops=flops, bytes_accessed=moved, transcendentals=0),
    )


COST = 400_000_000


def fast_device(sizes, phase, velocity):
    cols, rows, rows_y, planes = sizes
    total_z = planes * rows
    half_z = 3 * total_z // 8
    modes_z = 2 * half_z
    kx_local = KC // cols
    a_local = kx_local // rows
    lanes = a_local * KY
    points = rows_y * planes
    scale_inv = 1.0 / (NX * NY * total_z)
    tx_f, tx_i, ty_f, ty_i, tz_f, tz_i = tables(cols, rows, rows_y, planes)
    f32, bf16 = jnp.float32, jnp.bfloat16

    def x_forward(fields):
        count = fields.shape[0]

        def body(field_ref, table_ref, out_ref):
            lines = jnp.swapaxes(field_ref[0], 0, 1).reshape(points, NX).astype(bf16)
            made = dot(table_ref[...], lines, ((1,), (1,))).astype(bf16)
            out_ref[...] = made.reshape(cols, 1, 2 * kx_local, points)

        return call(
            body,
            (count,),
            [pl.BlockSpec((1, rows_y, planes, NX), lambda i: (i, 0, 0, 0)), whole(tx_f)],
            pl.BlockSpec((cols, 1, 2 * kx_local, points), lambda i: (0, i, 0, 0)),
            jax.ShapeDtypeStruct((cols, count, 2 * kx_local, points), bf16),
            COST * count,
            1 << 20,
        )(fields, tx_f)

    def y_forward(incoming):
        count = incoming.shape[1]

        def body(in_ref, table_ref, out_ref):
            lhs = jnp.concatenate(
                [
                    jnp.concatenate(
                        [in_ref[c, 0, :, z * rows_y : (z + 1) * rows_y] for c in range(cols)], axis=1
                    )
                    for z in range(planes)
                ],
                axis=0,
            )
            made = dot(lhs, table_ref[...]).reshape(planes, 2 * kx_local, 2 * KY)
            first, second = made[:, :kx_local], made[:, kx_local:]
            real = jnp.swapaxes(first[:, :, :KY] + second[:, :, KY:], 0, 1)
            imag = jnp.swapaxes(second[:, :, :KY] - first[:, :, KY:], 0, 1)
            both = jnp.concatenate([real, imag], axis=1).astype(bf16)
            for a in range(kx_local):
                r, k = a // a_local, a % a_local
                out_ref[r, 0, :, k * KY : (k + 1) * KY] = both[a]

        return call(
            body,
            (count,),
            [pl.BlockSpec((cols, 1, 2 * kx_local, points), lambda i: (0, i, 0, 0)), whole(ty_f)],
            pl.BlockSpec((rows, 1, 2 * planes, lanes), lambda i: (0, i, 0, 0)),
            jax.ShapeDtypeStruct((rows, count, 2 * planes, lanes), bf16),
            COST * count,
            1 << 20,
        )(incoming, ty_f)

    def y_inverse(incoming):
        count = incoming.shape[1]

        def body(in_ref, table_ref, out_ref):
            lhs = jnp.concatenate(
                [
                    in_ref[r, 0, :, k * KY : (k + 1) * KY]
                    for r in range(rows)
                    for k in range(a_local)
                ],
                axis=0,
            )
            made = dot(lhs, table_ref[...]).reshape(kx_local, 2 * planes, 2 * NY)
            first, second = made[:, :planes], made[:, planes:]
            real = jnp.swapaxes(first[:, :, :NY] - second[:, :, NY:], 0, 1)
            imag = jnp.swapaxes(first[:, :, NY:] + second[:, :, :NY], 0, 1)
            both = jnp.concatenate([real, imag], axis=1).astype(bf16)
            for c in range(cols):
                out_ref[c, 0] = jnp.concatenate(
                    [both[z, :, c * rows_y : (c + 1) * rows_y] for z in range(planes)], axis=1
                )

        return call(
            body,
            (count,),
            [pl.BlockSpec((rows, 1, 2 * planes, lanes), lambda i: (0, i, 0, 0)), whole(ty_i)],
            pl.BlockSpec((cols, 1, 2 * kx_local, points), lambda i: (0, i, 0, 0)),
            jax.ShapeDtypeStruct((cols, count, 2 * kx_local, points), bf16),
            COST * count,
            1 << 20,
        )(incoming, ty_i)

    def x_inverse(incoming):
        count = incoming.shape[1]

        def body(in_ref, table_ref, out_ref):
            lines = in_ref[...].reshape(2 * KC, points)
            made = dot(lines, table_ref[...], ((0,), (0,)))
            out_ref[0] = jnp.swapaxes(made.reshape(planes, rows_y, NX), 0, 1)

        return call(
            body,
            (count,),
            [pl.BlockSpec((cols, 1, 2 * kx_local, points), lambda i: (0, i, 0, 0)), whole(tx_i)],
            pl.BlockSpec((1, rows_y, planes, NX), lambda i: (i, 0, 0, 0)),
            jax.ShapeDtypeStruct((count, rows_y, planes, NX), f32),
            COST * count,
            1 << 20,
        )(incoming, tx_i)

    def over_col(values):
        return lax.all_to_all(values, "col", split_axis=0, concat_axis=0, tiled=True)

    def over_row(values):
        return lax.all_to_all(values, "row", split_axis=0, concat_axis=0, tiled=True)

    def forward(fields):
        return over_row(y_forward(over_col(x_forward(fields))))

    def inverse(outgoing):
        return x_inverse(over_col(y_inverse(over_row(outgoing))))

    cut = KY
    steps = lanes // cut
    first_a = lax.axis_index("col") * kx_local + lax.axis_index("row") * a_local
    wave_x = first_a.astype(f32) + jnp.repeat(jnp.arange(a_local, dtype=f32), KY)
    wave_y = jnp.tile(jnp.arange(KY, dtype=f32) - KC, a_local)
    wave_xy = jnp.stack([wave_x, wave_y])

    def coefficient(in_ref, f, table_ref):
        stacked = jnp.concatenate([in_ref[r, f] for r in range(rows)], axis=0)
        return dot(table_ref[...], stacked) * scale_inv

    def emit(out_ref, f, real, imag, table_ref):
        both = jnp.concatenate([real, imag], axis=0).astype(bf16)
        made = dot(table_ref[...], both).astype(bf16)
        for r in range(rows):
            out_ref[r, f] = made[r * 2 * planes : (r + 1) * 2 * planes]

    def waves(wave_ref):
        wx, wy = wave_ref[0:1, :], wave_ref[1:2, :]
        m = lax.broadcasted_iota(jnp.int32, (modes_z, cut), 0) - half_z
        wz = m.astype(f32) * (NX / total_z)
        return wx, wy, wz, wx * wx + wy * wy + wz * wz

    def lines_spec(count):
        return pl.BlockSpec((rows, count, 2 * planes, cut), lambda i: (0, 0, 0, i))

    def coeff_spec(count):
        return pl.BlockSpec((count, 2 * modes_z, cut), lambda i: (0, 0, i))

    def lines_shape(count):
        return jax.ShapeDtypeStruct((rows, count, 2 * planes, lanes), bf16)

    def coeff_shape(count):
        return jax.ShapeDtypeStruct((count, 2 * modes_z, lanes), f32)

    wave_spec = pl.BlockSpec((2, cut), lambda i: (0, i))

    def phase_spectral(in_ref, wave_ref, f_ref, i_ref, coeff_ref, out_ref):
        wx, wy, wz, k2 = waves(wave_ref)
        c = coefficient(in_ref, 0, f_ref)
        coeff_ref[0] = c
        re, im = c[:modes_z], c[modes_z:]
        emit(out_ref, 0, -(wx * im), wx * re, i_ref)
        emit(out_ref, 1, -(wy * im), wy * re, i_ref)
        emit(out_ref, 2, -(wz * im), wz * re, i_ref)
        emit(out_ref, 3, -k2 * re, -k2 * im, i_ref)

    def flow_spectral(in_ref, wave_ref, f_ref, i_ref, coeff_ref, out_ref):
        wx, wy, wz, _ = waves(wave_ref)
        cs = [coefficient(in_ref, j, f_ref) for j in range(3)]
        for j in range(3):
            coeff_ref[j] = cs[j]
        re, im = [c[:modes_z] for c in cs], [c[modes_z:] for c in cs]
        w = [wx, wy, wz]
        for j in range(3):
            p, q = (j + 1) % 3, (j + 2) % 3
            emit(
                out_ref,
                j,
                -(w[p] * im[q] - w[q] * im[p]),
                w[p] * re[q] - w[q] * re[p],
                i_ref,
            )

    def phase_solve(adv_ref, bulk_ref, old_ref, wave_ref, f_ref, i_ref, out_ref):
        wx, wy, wz, k2 = waves(wave_ref)
        adv = coefficient(adv_ref, 0, f_ref)
        bulk = coefficient(bulk_ref, 0, f_ref)
        old = old_ref[0]
        mean_mode = (wx == 0) & (wy == 0) & (wz == 0)
        stable = 1.0 / time_step + mobility * stabilizer * k2
        below = stable + mobility * epsilon * epsilon * k2 * k2
        parts = []
        for p in range(2):
            at = slice(p * modes_z, (p + 1) * modes_z)
            kept = jnp.where(mean_mode, 0.0, adv[at])
            parts.append((stable * old[at] - kept - mobility * k2 * bulk[at]) / below)
        emit(out_ref, 0, parts[0], parts[1], i_ref)

    def flow_solve(force_ref, old_ref, wave_ref, f_ref, i_ref, out_ref):
        wx, wy, wz, k2 = waves(wave_ref)
        viscous = 1.0 / time_step + k2 / reynolds
        largest = jnp.maximum(k2, 1.0)
        w = [wx, wy, wz]
        force = [coefficient(force_ref, j, f_ref) for j in range(3)]
        made = [[], [], []]
        for p in range(2):
            at = slice(p * modes_z, (p + 1) * modes_z)
            free = [(old_ref[j, at] / time_step + force[j][at]) / viscous for j in range(3)]
            normal = (wx * free[0] + wy * free[1] + wz * free[2]) / largest
            for j in range(3):
                made[j].append(free[j] - w[j] * normal)
        for j in range(3):
            emit(out_ref, j, made[j][0], made[j][1], i_ref)

    phase_lines = forward(phase[None])
    flow_lines = forward(velocity)
    bulk_field = phase * phase * phase - phase
    bulk_lines = forward(bulk_field[None])
    tail = [wave_spec, whole(tz_f), whole(tz_i)]
    last = (wave_xy, tz_f, tz_i)
    coeff_phase, gradient_lines = call(
        phase_spectral, (steps,), [lines_spec(1)] + tail,
        [coeff_spec(1), lines_spec(4)], [coeff_shape(1), lines_shape(4)], COST, 1 << 20,
    )(phase_lines, *last)
    coeff_flow, vortex_lines = call(
        flow_spectral, (steps,), [lines_spec(3)] + tail,
        [coeff_spec(3), lines_spec(3)], [coeff_shape(3), lines_shape(3)], COST, 1 << 20,
    )(flow_lines, *last)
    leading = inverse(gradient_lines)
    vortex = inverse(vortex_lines)
    advect, _, potential = phase_terms(phase, velocity, leading[0:3], leading[3])
    advect_lines = forward(advect[None])
    force_lines = forward(momentum(velocity, vortex, leading[0:3], potential))
    new_phase = call(
        phase_solve, (steps,), [lines_spec(1), lines_spec(1), coeff_spec(1)] + tail,
        lines_spec(1), lines_shape(1), COST, 1 << 20,
    )(advect_lines, bulk_lines, coeff_phase, *last)
    new_flow = call(
        flow_solve, (steps,), [lines_spec(3), coeff_spec(3)] + tail,
        lines_spec(3), lines_shape(3), COST, 1 << 20,
    )(force_lines, coeff_flow, *last)
    return (inverse(new_phase)[0], inverse(new_flow))


def solution(mesh):
    cols, rows = mesh.shape["col"], mesh.shape["row"]

    def on_device(phase, velocity):
        rows_y, planes = phase.shape[0], phase.shape[1]
        kx_local = KC // cols
        aligned = planes % 8 == 0 and kx_local % (8 * rows // math.gcd(8, rows)) == 0
        if aligned and (rows_y * planes) % 128 == 0:
            return fast_device((cols, rows, rows_y, planes), phase, velocity)
        return plain_device(phase, velocity)

    return jax.shard_map(
        on_device,
        mesh=mesh,
        in_specs=(P("col", "row", None), P(None, "col", "row", None)),
        out_specs=(P("col", "row", None), P(None, "col", "row", None)),
        check_vma=False,
    )
```

```python
import math

import jax
import jax.numpy as jnp
import ml_dtypes
import numpy as np
from jax import lax
from jax.experimental import pallas as pl
from jax.experimental.pallas import tpu as pltpu
from jax.sharding import PartitionSpec as P

NX = 512
NY = 512
KC = 192
KY = 384


time_step = 0.001
epsilon = 0.01
mobility = 1.0
reynolds = 100.0
stabilizer = 2.0


def cos_sin(row_index, col_index, period):
    residue = row_index[:, None] * col_index[None, :] % period
    angles = residue.astype(jnp.float32) * (2.0 * math.pi / period)
    return jnp.stack([jnp.cos(angles), jnp.sin(angles)]).astype(jnp.bfloat16)


def pair_sum(pieces, direction, stack_axis):
    if direction < 0:
        real_part = pieces[0, 0] + pieces[1, 1]
        imag_part = pieces[1, 0] - pieces[0, 1]
    else:
        real_part = pieces[0, 0] - pieces[1, 1]
        imag_part = pieces[0, 1] + pieces[1, 0]
    return jnp.stack([real_part, imag_part], axis=stack_axis)


def times_i(values):
    return jnp.stack([-values[:, 1], values[:, 0]], axis=1)


def phase_terms(phase, velocity, gradient, lap_field):
    advect = velocity[0] * gradient[0] + velocity[1] * gradient[1] + velocity[2] * gradient[2]
    bulk_term = phase * phase * phase - phase
    potential = bulk_term - epsilon * epsilon * lap_field
    return (advect, bulk_term, potential)


def momentum(velocity, vortex, gradient, potential):
    return jnp.stack(
        [
            velocity[1] * vortex[2] - velocity[2] * vortex[1] + potential * gradient[0],
            velocity[2] * vortex[0] - velocity[0] * vortex[2] + potential * gradient[1],
            velocity[0] * vortex[1] - velocity[1] * vortex[0] + potential * gradient[2],
        ]
    )


def plain_device(phase, velocity):
    col_count = lax.axis_size("col")
    row_count = lax.axis_size("row")
    rows_y = phase.shape[0]
    planes = phase.shape[1]
    total_z = planes * row_count
    half_z = 3 * total_z // 8
    modes_z = 2 * half_z
    kx_local = KC // col_count
    ky_local = KY // row_count
    scale_inv = 1.0 / (NX * NY * total_z)
    table_x = cos_sin(jnp.arange(NX, dtype=jnp.int32), jnp.arange(KC, dtype=jnp.int32), NX)
    table_y = cos_sin(jnp.arange(NY, dtype=jnp.int32), jnp.arange(KY, dtype=jnp.int32) - KC, NY)
    table_z = cos_sin(
        jnp.arange(total_z, dtype=jnp.int32), jnp.arange(modes_z, dtype=jnp.int32) - half_z, total_z
    )
    y_forward = table_y.reshape(2, col_count, rows_y, KY)
    y_inverse = table_y.reshape(2, col_count, rows_y, row_count, ky_local)
    z_table = table_z.reshape(2, row_count, planes, modes_z)
    weight = jnp.where(jnp.arange(KC) == 0, 1.0, 2.0).astype(jnp.bfloat16)[:, None, None, None]

    def along_y(incoming):
        field_count = incoming.shape[1]
        shaped = incoming.reshape(incoming.shape[0], field_count, col_count, 2, rows_y, planes)
        pieces = jnp.einsum(
            "afcpyz,tcyb->ptafbz", shaped, y_forward, preferred_element_type=jnp.float32
        )
        joined = pair_sum(pieces, -1, 2).astype(jnp.bfloat16)
        return joined.reshape(incoming.shape[0], field_count, 2, KY * planes)

    def along_z(incoming):
        field_count = incoming.shape[1]
        shaped = incoming.reshape(incoming.shape[0], field_count, 2, row_count, ky_local, planes)
        pieces = jnp.einsum(
            "afprbz,trzm->ptafbm", shaped, z_table, preferred_element_type=jnp.float32
        )
        joined = pair_sum(pieces, -1, 2) * scale_inv
        return joined.reshape(incoming.shape[0], field_count, 2, ky_local * modes_z)

    def back_y(incoming):
        field_count = incoming.shape[1]
        shaped = incoming.reshape(incoming.shape[0], field_count, 2, row_count, planes, ky_local)
        pieces = jnp.einsum(
            "afprzb,tcyrb->ptafcyz", shaped, y_inverse, preferred_element_type=jnp.float32
        )
        joined = pair_sum(pieces, 1, 3).astype(jnp.bfloat16)
        return joined.reshape(incoming.shape[0], field_count, col_count * 2 * rows_y * planes)

    def back_x(incoming):
        field_count = incoming.shape[1]
        shaped = incoming.reshape(KC, field_count, 2, rows_y, planes)
        scaled = jnp.stack([shaped[:, :, 0] * weight, -(shaped[:, :, 1] * weight)], axis=2)
        return jnp.einsum("afpyz,pxa->fyzx", scaled, table_x, preferred_element_type=jnp.float32)

    def forward(fields):
        field_count = fields.shape[0]
        pieces = jnp.einsum(
            "fyzx,txa->tafyz",
            fields.astype(jnp.bfloat16),
            table_x,
            preferred_element_type=jnp.float32,
        )
        x_lines = jnp.stack([pieces[0], -pieces[1]], axis=2).astype(jnp.bfloat16)
        x_lines = x_lines.reshape(KC, field_count, 2 * rows_y * planes)
        spread = along_y(lax.all_to_all(x_lines, "col", split_axis=0, concat_axis=2, tiled=True))
        return along_z(lax.all_to_all(spread, "row", split_axis=3, concat_axis=3, tiled=True))

    def inverse(spectra):
        field_count = spectra.shape[1]
        shaped = spectra.astype(jnp.bfloat16).reshape(kx_local, field_count, 2, ky_local, modes_z)
        pieces = jnp.einsum(
            "afpbm,trzm->ptafrzb", shaped, z_table, preferred_element_type=jnp.float32
        )
        z_planes = (
            pair_sum(pieces, 1, 2)
            .astype(jnp.bfloat16)
            .reshape(kx_local, field_count, 2, total_z * ky_local)
        )
        spread = back_y(lax.all_to_all(z_planes, "row", split_axis=3, concat_axis=3, tiled=True))
        return back_x(lax.all_to_all(spread, "col", split_axis=2, concat_axis=0, tiled=True))

    spectra = forward(jnp.concatenate([phase[None], velocity], axis=0))
    wave_x = (lax.axis_index("col") * kx_local + jnp.arange(kx_local, dtype=jnp.int32)).astype(
        jnp.float32
    )[:, None, None]
    modes_y = lax.axis_index("row") * ky_local + jnp.arange(ky_local, dtype=jnp.int32) - KC
    wave_y = jnp.broadcast_to(modes_y.astype(jnp.float32)[:, None], (ky_local, modes_z)).reshape(-1)
    z_values = (jnp.arange(modes_z, dtype=jnp.int32) - half_z).astype(jnp.float32) * (NX / total_z)
    wave_z = jnp.broadcast_to(z_values[None, :], (ky_local, modes_z)).reshape(-1)
    squared = wave_x * wave_x + wave_y * wave_y + wave_z * wave_z
    coeff_phase = spectra[:, 0]
    coeff_u = spectra[:, 1]
    coeff_v = spectra[:, 2]
    coeff_w = spectra[:, 3]
    gradients = [
        times_i(wave_x * coeff_phase),
        times_i(wave_y * coeff_phase),
        times_i(wave_z * coeff_phase),
    ]
    laplace = -squared * coeff_phase
    vortex_hat = [
        times_i(wave_y * coeff_w - wave_z * coeff_v),
        times_i(wave_z * coeff_u - wave_x * coeff_w),
        times_i(wave_x * coeff_v - wave_y * coeff_u),
    ]
    leading = inverse(jnp.stack(gradients + [laplace], axis=1))
    advect, bulk_term, potential = phase_terms(phase, velocity, leading[0:3], leading[3])
    phase_side = forward(jnp.stack([advect, bulk_term]))
    vortex = inverse(jnp.stack(vortex_hat, axis=1))
    flow_side = forward(momentum(velocity, vortex, leading[0:3], potential))
    nonlinear = jnp.concatenate([phase_side, flow_side], axis=1)
    mean_mode = (wave_x == 0) & (wave_y == 0) & (wave_z == 0)
    advect_hat = jnp.where(mean_mode, 0.0, nonlinear[:, 0])
    bulk_hat = nonlinear[:, 1]
    stable_part = 1.0 / time_step + mobility * stabilizer * squared
    new_phase = (stable_part * coeff_phase - advect_hat - mobility * squared * bulk_hat) / (
        stable_part + mobility * epsilon * epsilon * squared * squared
    )
    viscous = 1.0 / time_step + squared / reynolds
    unprojected = [
        (spectra[:, 1 + j] / time_step + nonlinear[:, 2 + j]) / viscous for j in range(3)
    ]
    normal_part = (
        wave_x * unprojected[0] + wave_y * unprojected[1] + wave_z * unprojected[2]
    ) / jnp.maximum(squared, 1.0)
    waves = [wave_x, wave_y, wave_z]
    new_flow = [unprojected[j] - waves[j] * normal_part for j in range(3)]
    result = inverse(jnp.stack([new_phase] + new_flow, axis=1))
    return (result[0], result[1:4])


def tables(cols, rows, rows_y, planes):
    total_z = planes * rows
    half_z = 3 * total_z // 8
    modes_z = 2 * half_z
    kx_local = KC // cols

    def pair(first, second, period):
        residue = first[:, None] * second[None, :] % period
        angles = residue.astype(np.float32) * np.float32(2.0 * math.pi / period)
        return [np.cos(angles).astype(ml_dtypes.bfloat16), np.sin(angles).astype(ml_dtypes.bfloat16)]

    cos_x, sin_x = pair(np.arange(KC), np.arange(NX), NX)
    cos_y, sin_y = pair(np.arange(NY), np.arange(KY) - KC, NY)
    cos_z, sin_z = pair(np.arange(total_z), np.arange(modes_z) - half_z, total_z)
    x_forward = np.stack([cos_x, -sin_x]).reshape(2, cols, kx_local, NX)
    x_forward = x_forward.transpose(1, 0, 2, 3).reshape(2 * KC, NX)
    weight = np.where(np.arange(KC) == 0, 1.0, 2.0).astype(ml_dtypes.bfloat16)[:, None]
    x_inverse = np.stack([cos_x * weight, -(sin_x * weight)]).reshape(2, cols, kx_local, NX)
    x_inverse = x_inverse.transpose(1, 0, 2, 3).reshape(2 * KC, NX)
    y_forward = np.concatenate([cos_y, sin_y], axis=1)
    y_inverse = np.concatenate([cos_y.T, sin_y.T], axis=1)
    cz, sz = (t.reshape(rows, planes, modes_z) for t in (cos_z, sin_z))
    z_forward = np.stack([np.stack([cz, sz], 1), np.stack([-sz, cz], 1)])
    z_forward = z_forward.transpose(0, 4, 1, 2, 3).reshape(2 * modes_z, 2 * total_z)
    z_inverse = np.stack([np.stack([cz, -sz], 2), np.stack([sz, cz], 2)], 1)
    z_inverse = z_inverse.reshape(2 * total_z, 2 * modes_z)
    return [jnp.asarray(t.astype(ml_dtypes.bfloat16)) for t in (x_forward, x_inverse, y_forward, y_inverse, z_forward, z_inverse)]


def dot(first, second, dims=((1,), (0,))):
    return lax.dot_general(first, second, (dims, ((), ())), preferred_element_type=jnp.float32)


def whole(array):
    return pl.BlockSpec(array.shape, lambda *_: (0,) * array.ndim)


def call(body, grid, in_specs, out_specs, out_shape, flops, moved, scratch=()):
    return pl.pallas_call(
        body,
        grid=grid,
        in_specs=in_specs,
        out_specs=out_specs,
        out_shape=out_shape,
        scratch_shapes=list(scratch),
        compiler_params=pltpu.CompilerParams(vmem_limit_bytes=40 * 1024 * 1024),
        cost_estimate=pl.CostEstimate(flops=flops, bytes_accessed=moved, transcendentals=0),
    )


COST = 400_000_000


def fast_device(sizes, phase, velocity):
    cols, rows, rows_y, planes = sizes
    total_z = planes * rows
    half_z = 3 * total_z // 8
    modes_z = 2 * half_z
    kx_local = KC // cols
    a_local = kx_local // rows
    lanes = a_local * KY
    points = rows_y * planes
    scale_inv = 1.0 / (NX * NY * total_z)
    tx_f, tx_i, ty_f, ty_i, tz_f, tz_i = tables(cols, rows, rows_y, planes)
    f32, bf16 = jnp.float32, jnp.bfloat16

    def x_forward(fields):
        count = fields.shape[0]

        def body(field_ref, table_ref, out_ref):
            lines = jnp.swapaxes(field_ref[0], 0, 1).reshape(points, NX).astype(bf16)
            made = dot(table_ref[...], lines, ((1,), (1,))).astype(bf16)
            out_ref[0] = made.reshape(cols, 2 * kx_local, points)

        return call(
            body,
            (count,),
            [pl.BlockSpec((1, rows_y, planes, NX), lambda i: (i, 0, 0, 0)), whole(tx_f)],
            pl.BlockSpec((1, cols, 2 * kx_local, points), lambda i: (i, 0, 0, 0)),
            jax.ShapeDtypeStruct((count, cols, 2 * kx_local, points), bf16),
            COST * count,
            1 << 20,
        )(fields, tx_f)

    def exchange(axis, size, src, dst, send, recv):
        me = lax.axis_index(axis)

        def copy(f, d):
            peer = lax.rem(me + d, size)
            return pltpu.make_async_remote_copy(
                src_ref=src.at[f, peer],
                dst_ref=dst.at[f, me],
                send_sem=send.at[f, d - 1],
                recv_sem=recv.at[f, d - 1],
                device_id={axis: peer},
                device_id_type=pl.DeviceIdType.MESH,
            )

        def start(f):
            for d in range(1, size):
                copy(f, d).start()

        def wait_recv(f):
            for d in range(1, size):
                copy(f, d).wait_recv()

        def wait_send(f):
            for d in range(1, size):
                copy(f, d).wait_send()

        def keep(f):
            dst[f, me] = src[f, me]

        return start, wait_recv, wait_send, keep

    def greet():
        barrier = pltpu.get_barrier_semaphore()
        for axis, size in (("col", cols), ("row", rows)):
            for d in range(1, size):
                peer = lax.rem(lax.axis_index(axis) + d, size)
                pl.semaphore_signal(
                    barrier, inc=1, device_id={axis: peer}, device_id_type=pl.DeviceIdType.MESH
                )
        pl.semaphore_wait(barrier, cols + rows - 2)

    def two_exchanges(incoming, table, first, second, compute, ident):
        count = incoming.shape[0]
        (axis1, size1, shape1), (axis2, size2, shape2) = first, second
        ahead = 2

        def body(in_ref, table_ref, out_ref, got, made, send1, recv1, send2, recv2):
            greet()
            start1, recv_1, sent1, keep1 = exchange(axis1, size1, in_ref, got, send1, recv1)
            start2, recv_2, sent2, keep2 = exchange(axis2, size2, made, out_ref, send2, recv2)
            for f in range(min(ahead, count)):
                start1(f)

            def step(f, carry):
                @pl.when(f + ahead < count)
                def _():
                    start1(f + ahead)

                keep1(f)
                recv_1(f)
                compute(f, got, table_ref, made)
                start2(f)
                keep2(f)
                return carry

            lax.fori_loop(0, count, step, 0)

            def finish(f, carry):
                recv_2(f)
                sent1(f)
                sent2(f)
                return carry

            lax.fori_loop(0, count, finish, 0)

        sems = pltpu.SemaphoreType.DMA
        return pl.pallas_call(
            body,
            in_specs=[pl.BlockSpec(memory_space=pltpu.VMEM)] * 2,
            out_specs=pl.BlockSpec(memory_space=pltpu.VMEM),
            out_shape=jax.ShapeDtypeStruct((count,) + shape2, bf16),
            scratch_shapes=[
                pltpu.VMEM((count,) + shape1, bf16),
                pltpu.VMEM((count,) + shape2, bf16),
                sems((count, size1 - 1)),
                sems((count, size1 - 1)),
                sems((count, size2 - 1)),
                sems((count, size2 - 1)),
            ],
            compiler_params=pltpu.CompilerParams(
                collective_id=ident, has_side_effects=True, vmem_limit_bytes=40 * 1024 * 1024
            ),
            cost_estimate=pl.CostEstimate(
                flops=COST * count, bytes_accessed=1 << 20, transcendentals=0
            ),
        )(incoming, table)

    col_side = ("col", cols, (cols, 2 * kx_local, points))
    row_side = ("row", rows, (rows, 2 * planes, lanes))

    def y_forward(f, in_ref, table_ref, out_ref):
        lhs = jnp.concatenate(
            [
                jnp.concatenate(
                    [in_ref[f, c, :, z * rows_y : (z + 1) * rows_y] for c in range(cols)], axis=1
                )
                for z in range(planes)
            ],
            axis=0,
        )
        made = dot(lhs, table_ref[...]).reshape(planes, 2 * kx_local, 2 * KY)
        first, second = made[:, :kx_local], made[:, kx_local:]
        real = jnp.swapaxes(first[:, :, :KY] + second[:, :, KY:], 0, 1)
        imag = jnp.swapaxes(second[:, :, :KY] - first[:, :, KY:], 0, 1)
        both = jnp.concatenate([real, imag], axis=1).astype(bf16)
        for a in range(kx_local):
            r, k = a // a_local, a % a_local
            out_ref[f, r, :, k * KY : (k + 1) * KY] = both[a]

    def y_inverse(f, in_ref, table_ref, out_ref):
        lhs = jnp.concatenate(
            [in_ref[f, r, :, k * KY : (k + 1) * KY] for r in range(rows) for k in range(a_local)],
            axis=0,
        )
        made = dot(lhs, table_ref[...]).reshape(kx_local, 2 * planes, 2 * NY)
        first, second = made[:, :planes], made[:, planes:]
        real = jnp.swapaxes(first[:, :, :NY] - second[:, :, NY:], 0, 1)
        imag = jnp.swapaxes(first[:, :, NY:] + second[:, :, :NY], 0, 1)
        both = jnp.concatenate([real, imag], axis=1).astype(bf16)
        for c in range(cols):
            out_ref[f, c] = jnp.concatenate(
                [both[z, :, c * rows_y : (c + 1) * rows_y] for z in range(planes)], axis=1
            )

    def to_spectral(x_lines, ident):
        return two_exchanges(x_lines, ty_f, col_side, row_side, y_forward, ident)

    def to_physical(z_lines, ident):
        return two_exchanges(z_lines, ty_i, row_side, col_side, y_inverse, ident)

    def x_forward_first():
        def body(phase_ref, flow_ref, table_ref, out_ref):
            i = pl.program_id(0)
            c = phase_ref[...]
            scalar = jnp.where(i == 0, c, c * c * c - c)
            field = jnp.where((i == 0) | (i == 4), scalar, flow_ref[0])
            lines = jnp.swapaxes(field, 0, 1).reshape(points, NX).astype(bf16)
            made = dot(table_ref[...], lines, ((1,), (1,))).astype(bf16)
            out_ref[0] = made.reshape(cols, 2 * kx_local, points)

        return call(
            body,
            (5,),
            [
                pl.BlockSpec((rows_y, planes, NX), lambda i: (0, 0, 0)),
                pl.BlockSpec((1, rows_y, planes, NX), lambda i: (jnp.clip(i - 1, 0, 2), 0, 0, 0)),
                whole(tx_f),
            ],
            pl.BlockSpec((1, cols, 2 * kx_local, points), lambda i: (i, 0, 0, 0)),
            jax.ShapeDtypeStruct((5, cols, 2 * kx_local, points), bf16),
            COST * 5,
            1 << 20,
        )(phase, velocity, tx_f)

    def x_inverse(incoming):
        count = incoming.shape[0]

        def body(in_ref, table_ref, out_ref):
            lines = in_ref[...].reshape(2 * KC, points)
            made = dot(lines, table_ref[...], ((0,), (0,)))
            out_ref[0] = jnp.swapaxes(made.reshape(planes, rows_y, NX), 0, 1)

        return call(
            body,
            (count,),
            [pl.BlockSpec((1, cols, 2 * kx_local, points), lambda i: (i, 0, 0, 0)), whole(tx_i)],
            pl.BlockSpec((1, rows_y, planes, NX), lambda i: (i, 0, 0, 0)),
            jax.ShapeDtypeStruct((count, rows_y, planes, NX), f32),
            COST * count,
            1 << 20,
        )(incoming, tx_i)

    cut = KY
    steps = lanes // cut
    first_a = lax.axis_index("col") * kx_local + lax.axis_index("row") * a_local
    wave_x = first_a.astype(f32) + jnp.repeat(jnp.arange(a_local, dtype=f32), KY)
    wave_y = jnp.tile(jnp.arange(KY, dtype=f32) - KC, a_local)
    wave_xy = jnp.stack([wave_x, wave_y])

    def coefficient(in_ref, f, table_ref):
        stacked = jnp.concatenate([in_ref[f, r] for r in range(rows)], axis=0)
        return dot(table_ref[...], stacked) * scale_inv

    def emit(out_ref, f, real, imag, table_ref):
        both = jnp.concatenate([real, imag], axis=0).astype(bf16)
        made = dot(table_ref[...], both).astype(bf16)
        for r in range(rows):
            out_ref[f, r] = made[r * 2 * planes : (r + 1) * 2 * planes]

    def waves(wave_ref):
        wx, wy = wave_ref[0:1, :], wave_ref[1:2, :]
        m = lax.broadcasted_iota(jnp.int32, (modes_z, cut), 0) - half_z
        wz = m.astype(f32) * (NX / total_z)
        return wx, wy, wz, wx * wx + wy * wy + wz * wz

    def lines_spec(count):
        return pl.BlockSpec((count, rows, 2 * planes, cut), lambda i: (0, 0, 0, i))

    def coeff_spec(count):
        return pl.BlockSpec((count, 2 * modes_z, cut), lambda i: (0, 0, i))

    def lines_shape(count):
        return jax.ShapeDtypeStruct((count, rows, 2 * planes, lanes), bf16)

    def coeff_shape(count):
        return jax.ShapeDtypeStruct((count, 2 * modes_z, lanes), f32)

    wave_spec = pl.BlockSpec((2, cut), lambda i: (0, i))

    def derive(in_ref, wave_ref, f_ref, i_ref, coeff_ref, out_ref):
        wx, wy, wz, k2 = waves(wave_ref)
        cs = [coefficient(in_ref, j, f_ref) for j in range(5)]
        for j in range(5):
            coeff_ref[j] = cs[j]
        re, im = [c[:modes_z] for c in cs], [c[modes_z:] for c in cs]
        emit(out_ref, 0, -(wx * im[0]), wx * re[0], i_ref)
        emit(out_ref, 1, -(wy * im[0]), wy * re[0], i_ref)
        emit(out_ref, 2, -(wz * im[0]), wz * re[0], i_ref)
        emit(out_ref, 3, -k2 * re[0], -k2 * im[0], i_ref)
        w = [wx, wy, wz]
        for j in range(3):
            p, q = (j + 1) % 3, (j + 2) % 3
            real = -(w[p] * im[1 + q] - w[q] * im[1 + p])
            emit(out_ref, 4 + j, real, w[p] * re[1 + q] - w[q] * re[1 + p], i_ref)

    def solve(in_ref, old_ref, wave_ref, f_ref, i_ref, out_ref):
        wx, wy, wz, k2 = waves(wave_ref)
        mean_mode = (wx == 0) & (wy == 0) & (wz == 0)
        stable = 1.0 / time_step + mobility * stabilizer * k2
        below = stable + mobility * epsilon * epsilon * k2 * k2
        viscous = 1.0 / time_step + k2 / reynolds
        largest = jnp.maximum(k2, 1.0)
        w = [wx, wy, wz]
        added = [coefficient(in_ref, j, f_ref) for j in range(4)]
        made = [[], [], [], []]
        for p in range(2):
            at = slice(p * modes_z, (p + 1) * modes_z)
            kept = jnp.where(mean_mode, 0.0, added[0][at])
            made[0].append((stable * old_ref[0, at] - kept - mobility * k2 * old_ref[4, at]) / below)
            free = [(old_ref[1 + j, at] / time_step + added[1 + j][at]) / viscous for j in range(3)]
            normal = (wx * free[0] + wy * free[1] + wz * free[2]) / largest
            for j in range(3):
                made[1 + j].append(free[j] - w[j] * normal)
        for j in range(4):
            emit(out_ref, j, made[j][0], made[j][1], i_ref)

    tail = [wave_spec, whole(tz_f), whole(tz_i)]
    last = (wave_xy, tz_f, tz_i)
    first_lines = to_spectral(x_forward_first(), 0)
    coeffs, derived = call(
        derive, (steps,), [lines_spec(5)] + tail,
        [coeff_spec(5), lines_spec(7)], [coeff_shape(5), lines_shape(7)], COST, 1 << 20,
    )(first_lines, *last)
    fields = x_inverse(to_physical(derived, 1))
    gradient, vortex = fields[0:3], fields[4:7]
    advect, _, potential = phase_terms(phase, velocity, gradient, fields[3])
    forcing = momentum(velocity, vortex, gradient, potential)
    products = jnp.concatenate([advect[None], forcing], axis=0)
    product_lines = to_spectral(x_forward(products), 2)
    solved = call(
        solve, (steps,), [lines_spec(4), coeff_spec(5)] + tail,
        lines_spec(4), lines_shape(4), COST, 1 << 20,
    )(product_lines, coeffs, *last)
    result = x_inverse(to_physical(solved, 3))
    return (result[0], result[1:4])


def solution(mesh):
    cols, rows = mesh.shape["col"], mesh.shape["row"]

    def on_device(phase, velocity):
        rows_y, planes = phase.shape[0], phase.shape[1]
        kx_local = KC // cols
        aligned = planes % 8 == 0 and kx_local % (8 * rows // math.gcd(8, rows)) == 0
        if aligned and (rows_y * planes) % 128 == 0:
            return fast_device((cols, rows, rows_y, planes), phase, velocity)
        return plain_device(phase, velocity)

    return jax.shard_map(
        on_device,
        mesh=mesh,
        in_specs=(P("col", "row", None), P(None, "col", "row", None)),
        out_specs=(P("col", "row", None), P(None, "col", "row", None)),
        check_vma=False,
    )
```

```python
import math

import jax
import jax.numpy as jnp
import ml_dtypes
import numpy as np
from jax import lax
from jax.experimental import pallas as pl
from jax.experimental.pallas import tpu as pltpu
from jax.sharding import PartitionSpec as P

NX = 512
NY = 512
KC = 192
KY = 384


time_step = 0.001
epsilon = 0.01
mobility = 1.0
reynolds = 100.0
stabilizer = 2.0


def cos_sin(row_index, col_index, period):
    residue = row_index[:, None] * col_index[None, :] % period
    angles = residue.astype(jnp.float32) * (2.0 * math.pi / period)
    return jnp.stack([jnp.cos(angles), jnp.sin(angles)]).astype(jnp.bfloat16)


def pair_sum(pieces, direction, stack_axis):
    if direction < 0:
        real_part = pieces[0, 0] + pieces[1, 1]
        imag_part = pieces[1, 0] - pieces[0, 1]
    else:
        real_part = pieces[0, 0] - pieces[1, 1]
        imag_part = pieces[0, 1] + pieces[1, 0]
    return jnp.stack([real_part, imag_part], axis=stack_axis)


def times_i(values):
    return jnp.stack([-values[:, 1], values[:, 0]], axis=1)


def phase_terms(phase, velocity, gradient, lap_field):
    advect = velocity[0] * gradient[0] + velocity[1] * gradient[1] + velocity[2] * gradient[2]
    bulk_term = phase * phase * phase - phase
    potential = bulk_term - epsilon * epsilon * lap_field
    return (advect, bulk_term, potential)


def momentum(velocity, vortex, gradient, potential):
    return jnp.stack(
        [
            velocity[1] * vortex[2] - velocity[2] * vortex[1] + potential * gradient[0],
            velocity[2] * vortex[0] - velocity[0] * vortex[2] + potential * gradient[1],
            velocity[0] * vortex[1] - velocity[1] * vortex[0] + potential * gradient[2],
        ]
    )


def plain_device(phase, velocity):
    col_count = lax.axis_size("col")
    row_count = lax.axis_size("row")
    rows_y = phase.shape[0]
    planes = phase.shape[1]
    total_z = planes * row_count
    half_z = 3 * total_z // 8
    modes_z = 2 * half_z
    kx_local = KC // col_count
    ky_local = KY // row_count
    scale_inv = 1.0 / (NX * NY * total_z)
    table_x = cos_sin(jnp.arange(NX, dtype=jnp.int32), jnp.arange(KC, dtype=jnp.int32), NX)
    table_y = cos_sin(jnp.arange(NY, dtype=jnp.int32), jnp.arange(KY, dtype=jnp.int32) - KC, NY)
    table_z = cos_sin(
        jnp.arange(total_z, dtype=jnp.int32), jnp.arange(modes_z, dtype=jnp.int32) - half_z, total_z
    )
    y_forward = table_y.reshape(2, col_count, rows_y, KY)
    y_inverse = table_y.reshape(2, col_count, rows_y, row_count, ky_local)
    z_table = table_z.reshape(2, row_count, planes, modes_z)
    weight = jnp.where(jnp.arange(KC) == 0, 1.0, 2.0).astype(jnp.bfloat16)[:, None, None, None]

    def along_y(incoming):
        field_count = incoming.shape[1]
        shaped = incoming.reshape(incoming.shape[0], field_count, col_count, 2, rows_y, planes)
        pieces = jnp.einsum(
            "afcpyz,tcyb->ptafbz", shaped, y_forward, preferred_element_type=jnp.float32
        )
        joined = pair_sum(pieces, -1, 2).astype(jnp.bfloat16)
        return joined.reshape(incoming.shape[0], field_count, 2, KY * planes)

    def along_z(incoming):
        field_count = incoming.shape[1]
        shaped = incoming.reshape(incoming.shape[0], field_count, 2, row_count, ky_local, planes)
        pieces = jnp.einsum(
            "afprbz,trzm->ptafbm", shaped, z_table, preferred_element_type=jnp.float32
        )
        joined = pair_sum(pieces, -1, 2) * scale_inv
        return joined.reshape(incoming.shape[0], field_count, 2, ky_local * modes_z)

    def back_y(incoming):
        field_count = incoming.shape[1]
        shaped = incoming.reshape(incoming.shape[0], field_count, 2, row_count, planes, ky_local)
        pieces = jnp.einsum(
            "afprzb,tcyrb->ptafcyz", shaped, y_inverse, preferred_element_type=jnp.float32
        )
        joined = pair_sum(pieces, 1, 3).astype(jnp.bfloat16)
        return joined.reshape(incoming.shape[0], field_count, col_count * 2 * rows_y * planes)

    def back_x(incoming):
        field_count = incoming.shape[1]
        shaped = incoming.reshape(KC, field_count, 2, rows_y, planes)
        scaled = jnp.stack([shaped[:, :, 0] * weight, -(shaped[:, :, 1] * weight)], axis=2)
        return jnp.einsum("afpyz,pxa->fyzx", scaled, table_x, preferred_element_type=jnp.float32)

    def forward(fields):
        field_count = fields.shape[0]
        pieces = jnp.einsum(
            "fyzx,txa->tafyz",
            fields.astype(jnp.bfloat16),
            table_x,
            preferred_element_type=jnp.float32,
        )
        x_lines = jnp.stack([pieces[0], -pieces[1]], axis=2).astype(jnp.bfloat16)
        x_lines = x_lines.reshape(KC, field_count, 2 * rows_y * planes)
        spread = along_y(lax.all_to_all(x_lines, "col", split_axis=0, concat_axis=2, tiled=True))
        return along_z(lax.all_to_all(spread, "row", split_axis=3, concat_axis=3, tiled=True))

    def inverse(spectra):
        field_count = spectra.shape[1]
        shaped = spectra.astype(jnp.bfloat16).reshape(kx_local, field_count, 2, ky_local, modes_z)
        pieces = jnp.einsum(
            "afpbm,trzm->ptafrzb", shaped, z_table, preferred_element_type=jnp.float32
        )
        z_planes = (
            pair_sum(pieces, 1, 2)
            .astype(jnp.bfloat16)
            .reshape(kx_local, field_count, 2, total_z * ky_local)
        )
        spread = back_y(lax.all_to_all(z_planes, "row", split_axis=3, concat_axis=3, tiled=True))
        return back_x(lax.all_to_all(spread, "col", split_axis=2, concat_axis=0, tiled=True))

    spectra = forward(jnp.concatenate([phase[None], velocity], axis=0))
    wave_x = (lax.axis_index("col") * kx_local + jnp.arange(kx_local, dtype=jnp.int32)).astype(
        jnp.float32
    )[:, None, None]
    modes_y = lax.axis_index("row") * ky_local + jnp.arange(ky_local, dtype=jnp.int32) - KC
    wave_y = jnp.broadcast_to(modes_y.astype(jnp.float32)[:, None], (ky_local, modes_z)).reshape(-1)
    z_values = (jnp.arange(modes_z, dtype=jnp.int32) - half_z).astype(jnp.float32) * (NX / total_z)
    wave_z = jnp.broadcast_to(z_values[None, :], (ky_local, modes_z)).reshape(-1)
    squared = wave_x * wave_x + wave_y * wave_y + wave_z * wave_z
    coeff_phase = spectra[:, 0]
    coeff_u = spectra[:, 1]
    coeff_v = spectra[:, 2]
    coeff_w = spectra[:, 3]
    gradients = [
        times_i(wave_x * coeff_phase),
        times_i(wave_y * coeff_phase),
        times_i(wave_z * coeff_phase),
    ]
    laplace = -squared * coeff_phase
    vortex_hat = [
        times_i(wave_y * coeff_w - wave_z * coeff_v),
        times_i(wave_z * coeff_u - wave_x * coeff_w),
        times_i(wave_x * coeff_v - wave_y * coeff_u),
    ]
    leading = inverse(jnp.stack(gradients + [laplace], axis=1))
    advect, bulk_term, potential = phase_terms(phase, velocity, leading[0:3], leading[3])
    phase_side = forward(jnp.stack([advect, bulk_term]))
    vortex = inverse(jnp.stack(vortex_hat, axis=1))
    flow_side = forward(momentum(velocity, vortex, leading[0:3], potential))
    nonlinear = jnp.concatenate([phase_side, flow_side], axis=1)
    mean_mode = (wave_x == 0) & (wave_y == 0) & (wave_z == 0)
    advect_hat = jnp.where(mean_mode, 0.0, nonlinear[:, 0])
    bulk_hat = nonlinear[:, 1]
    stable_part = 1.0 / time_step + mobility * stabilizer * squared
    new_phase = (stable_part * coeff_phase - advect_hat - mobility * squared * bulk_hat) / (
        stable_part + mobility * epsilon * epsilon * squared * squared
    )
    viscous = 1.0 / time_step + squared / reynolds
    unprojected = [
        (spectra[:, 1 + j] / time_step + nonlinear[:, 2 + j]) / viscous for j in range(3)
    ]
    normal_part = (
        wave_x * unprojected[0] + wave_y * unprojected[1] + wave_z * unprojected[2]
    ) / jnp.maximum(squared, 1.0)
    waves = [wave_x, wave_y, wave_z]
    new_flow = [unprojected[j] - waves[j] * normal_part for j in range(3)]
    result = inverse(jnp.stack([new_phase] + new_flow, axis=1))
    return (result[0], result[1:4])


def tables(cols, rows, rows_y, planes):
    total_z = planes * rows
    half_z = 3 * total_z // 8
    modes_z = 2 * half_z
    kx_local = KC // cols

    def pair(first, second, period):
        residue = first[:, None] * second[None, :] % period
        angles = residue.astype(np.float32) * np.float32(2.0 * math.pi / period)
        return [np.cos(angles).astype(ml_dtypes.bfloat16), np.sin(angles).astype(ml_dtypes.bfloat16)]

    cos_x, sin_x = pair(np.arange(KC), np.arange(NX), NX)
    cos_y, sin_y = pair(np.arange(NY), np.arange(KY) - KC, NY)
    cos_z, sin_z = pair(np.arange(total_z), np.arange(modes_z) - half_z, total_z)
    x_forward = np.stack([cos_x, -sin_x]).reshape(2, cols, kx_local, NX)
    x_forward = x_forward.transpose(1, 0, 2, 3).reshape(2 * KC, NX)
    weight = np.where(np.arange(KC) == 0, 1.0, 2.0).astype(ml_dtypes.bfloat16)[:, None]
    x_inverse = np.stack([cos_x * weight, -(sin_x * weight)]).reshape(2, cols, kx_local, NX)
    x_inverse = x_inverse.transpose(1, 0, 2, 3).reshape(2 * KC, NX)
    y_forward = np.concatenate([cos_y, sin_y], axis=1)
    y_inverse = np.concatenate([cos_y.T, sin_y.T], axis=1)
    cz, sz = (t.reshape(rows, planes, modes_z) for t in (cos_z, sin_z))
    z_forward = np.stack([np.stack([cz, sz], 1), np.stack([-sz, cz], 1)])
    z_forward = z_forward.transpose(0, 4, 1, 2, 3).reshape(2 * modes_z, 2 * total_z)
    z_inverse = np.stack([np.stack([cz, -sz], 2), np.stack([sz, cz], 2)], 1)
    z_inverse = z_inverse.reshape(2 * total_z, 2 * modes_z)
    return [jnp.asarray(t.astype(ml_dtypes.bfloat16)) for t in (x_forward, x_inverse, y_forward, y_inverse, z_forward, z_inverse)]


def dot(first, second, dims=((1,), (0,))):
    return lax.dot_general(first, second, (dims, ((), ())), preferred_element_type=jnp.float32)


def whole(array):
    return pl.BlockSpec(array.shape, lambda *_: (0,) * array.ndim)


def call(body, grid, in_specs, out_specs, out_shape, flops, moved, scratch=()):
    return pl.pallas_call(
        body,
        grid=grid,
        in_specs=in_specs,
        out_specs=out_specs,
        out_shape=out_shape,
        scratch_shapes=list(scratch),
        compiler_params=pltpu.CompilerParams(vmem_limit_bytes=40 * 1024 * 1024),
        cost_estimate=pl.CostEstimate(flops=flops, bytes_accessed=moved, transcendentals=0),
    )


COST = 400_000_000


def fast_device(sizes, phase, velocity):
    cols, rows, rows_y, planes = sizes
    total_z = planes * rows
    half_z = 3 * total_z // 8
    modes_z = 2 * half_z
    kx_local = KC // cols
    a_local = kx_local // rows
    lanes = a_local * KY
    points = rows_y * planes
    scale_inv = 1.0 / (NX * NY * total_z)
    tx_f, tx_i, ty_f, ty_i, tz_f, tz_i = tables(cols, rows, rows_y, planes)
    f32, bf16 = jnp.float32, jnp.bfloat16

    def exchange(axis, size, src, dst, send, recv):
        me = lax.axis_index(axis)

        def copy(f, d):
            peer = lax.rem(me + d, size)
            return pltpu.make_async_remote_copy(
                src_ref=src.at[f, peer],
                dst_ref=dst.at[f, me],
                send_sem=send.at[f, d - 1],
                recv_sem=recv.at[f, d - 1],
                device_id={axis: peer},
                device_id_type=pl.DeviceIdType.MESH,
            )

        def start(f):
            for d in range(1, size):
                copy(f, d).start()

        def wait_recv(f):
            for d in range(1, size):
                copy(f, d).wait_recv()

        def wait_send(f):
            for d in range(1, size):
                copy(f, d).wait_send()

        def keep(f):
            dst[f, me] = src[f, me]

        return start, wait_recv, wait_send, keep

    def greet():
        barrier = pltpu.get_barrier_semaphore()
        for axis, size in (("col", cols), ("row", rows)):
            for d in range(1, size):
                peer = lax.rem(lax.axis_index(axis) + d, size)
                pl.semaphore_signal(
                    barrier, inc=1, device_id={axis: peer}, device_id_type=pl.DeviceIdType.MESH
                )
        pl.semaphore_wait(barrier, cols + rows - 2)

    def two_exchanges(operands, count, first, second, prepare, compute, unfold, ident):
        (axis1, size1, shape1), (axis2, size2, shape2) = first, second
        ins = len(operands)

        def body(*refs):
            in_refs, out_ref = refs[:ins], refs[ins]
            got, made, send1, recv1, send2, recv2 = refs[ins + 1 : ins + 7]
            more = list(refs[ins + 7 :])
            source = more.pop(0) if prepare else in_refs[0]
            landed = more.pop(0) if unfold else out_ref
            start1, recv_1, sent1, keep1 = exchange(axis1, size1, source, got, send1, recv1)
            start2, recv_2, sent2, keep2 = exchange(axis2, size2, made, landed, send2, recv2)
            if prepare:
                prepare(0, in_refs, source)
            greet()
            start1(0)

            def begin(f, carry):
                if prepare:
                    prepare(f, in_refs, source)
                start1(f)
                return carry

            lax.fori_loop(1, count, begin, 0)

            def step(f, carry):
                keep1(f)
                recv_1(f)
                compute(f, got, in_refs, made)
                start2(f)
                keep2(f)
                return carry

            lax.fori_loop(0, count, step, 0)

            def finish(f, carry):
                recv_2(f)
                if unfold:
                    unfold(f, landed, in_refs, out_ref)
                sent1(f)
                sent2(f)
                return carry

            lax.fori_loop(0, count, finish, 0)

        sems = pltpu.SemaphoreType.DMA
        scratch = [
            pltpu.VMEM((count,) + shape1, bf16),
            pltpu.VMEM((count,) + shape2, bf16),
            sems((count, size1 - 1)),
            sems((count, size1 - 1)),
            sems((count, size2 - 1)),
            sems((count, size2 - 1)),
        ]
        if prepare:
            scratch.append(pltpu.VMEM((count,) + shape1, bf16))
        if unfold:
            scratch.append(pltpu.VMEM((count,) + shape2, bf16))
            out_shape = jax.ShapeDtypeStruct((count, rows_y, planes, NX), f32)
        else:
            out_shape = jax.ShapeDtypeStruct((count,) + shape2, bf16)
        return pl.pallas_call(
            body,
            in_specs=[pl.BlockSpec(memory_space=pltpu.VMEM)] * ins,
            out_specs=pl.BlockSpec(memory_space=pltpu.VMEM),
            out_shape=out_shape,
            scratch_shapes=scratch,
            compiler_params=pltpu.CompilerParams(
                collective_id=ident, has_side_effects=True, vmem_limit_bytes=40 * 1024 * 1024
            ),
            cost_estimate=pl.CostEstimate(
                flops=COST * count, bytes_accessed=1 << 20, transcendentals=0
            ),
        )(*operands)

    col_side = ("col", cols, (cols, 2 * kx_local, points))
    row_side = ("row", rows, (rows, 2 * planes, lanes))

    def y_forward(f, in_ref, in_refs, out_ref):
        table_ref = in_refs[-1]
        lhs = jnp.concatenate(
            [
                jnp.concatenate(
                    [in_ref[f, c, :, z * rows_y : (z + 1) * rows_y] for c in range(cols)], axis=1
                )
                for z in range(planes)
            ],
            axis=0,
        )
        made = dot(lhs, table_ref[...]).reshape(planes, 2 * kx_local, 2 * KY)
        first, second = made[:, :kx_local], made[:, kx_local:]
        real = jnp.swapaxes(first[:, :, :KY] + second[:, :, KY:], 0, 1)
        imag = jnp.swapaxes(second[:, :, :KY] - first[:, :, KY:], 0, 1)
        both = jnp.concatenate([real, imag], axis=1).astype(bf16)
        for a in range(kx_local):
            r, k = a // a_local, a % a_local
            out_ref[f, r, :, k * KY : (k + 1) * KY] = both[a]

    def y_inverse(f, in_ref, in_refs, out_ref):
        table_ref = in_refs[-1]
        lhs = jnp.concatenate(
            [in_ref[f, r, :, k * KY : (k + 1) * KY] for r in range(rows) for k in range(a_local)],
            axis=0,
        )
        made = dot(lhs, table_ref[...]).reshape(kx_local, 2 * planes, 2 * NY)
        first, second = made[:, :planes], made[:, planes:]
        real = jnp.swapaxes(first[:, :, :NY] - second[:, :, NY:], 0, 1)
        imag = jnp.swapaxes(first[:, :, NY:] + second[:, :, :NY], 0, 1)
        both = jnp.concatenate([real, imag], axis=1).astype(bf16)
        for c in range(cols):
            out_ref[f, c] = jnp.concatenate(
                [both[z, :, c * rows_y : (c + 1) * rows_y] for z in range(planes)], axis=1
            )

    def x_lines(field, table_ref):
        lines = jnp.swapaxes(field, 0, 1).reshape(points, NX).astype(bf16)
        made = dot(table_ref[...], lines, ((1,), (1,))).astype(bf16)
        return made.reshape(cols, 2 * kx_local, points)

    def x_field(lines, table_ref):
        made = dot(lines.reshape(2 * KC, points), table_ref[...], ((0,), (0,)))
        return jnp.swapaxes(made.reshape(planes, rows_y, NX), 0, 1)

    def first_to_spectral():
        def prepare(f, in_refs, source):
            phase_ref, flow_ref, table_ref, _ = in_refs
            if isinstance(f, int):
                source[f] = x_lines(phase_ref[...], table_ref)
                return

            @pl.when(f < 4)
            def _():
                source[f] = x_lines(flow_ref[jnp.minimum(f - 1, 2)], table_ref)

            @pl.when(f == 4)
            def _():
                c = phase_ref[...]
                source[f] = x_lines(c * c * c - c, table_ref)

        operands = (phase, velocity, tx_f, ty_f)
        return two_exchanges(operands, 5, col_side, row_side, prepare, y_forward, None, 0)

    def products_to_spectral(products):
        def prepare(f, in_refs, source):
            source[f] = x_lines(in_refs[0][f], in_refs[1])

        operands = (products, tx_f, ty_f)
        return two_exchanges(operands, 4, col_side, row_side, prepare, y_forward, None, 2)

    def derived_to_physical(derived):
        def unfold(f, landed, in_refs, out_ref):
            out_ref[f] = x_field(landed[f], in_refs[1])

        operands = (derived, tx_i, ty_i)
        return two_exchanges(operands, 7, row_side, col_side, None, y_inverse, unfold, 1)

    def solved_to_lines(solved):
        return two_exchanges((solved, ty_i), 4, row_side, col_side, None, y_inverse, None, 3)

    def x_inverse(incoming, begin, count):
        def body(in_ref, table_ref, out_ref):
            out_ref[0] = x_field(in_ref[0], table_ref)

        return call(
            body,
            (count,),
            [
                pl.BlockSpec((1, cols, 2 * kx_local, points), lambda i: (i + begin, 0, 0, 0)),
                whole(tx_i),
            ],
            pl.BlockSpec((1, rows_y, planes, NX), lambda i: (i, 0, 0, 0)),
            jax.ShapeDtypeStruct((count, rows_y, planes, NX), f32),
            COST * count,
            1 << 20,
        )(incoming, tx_i)

    cut = KY
    steps = lanes // cut
    first_a = lax.axis_index("col") * kx_local + lax.axis_index("row") * a_local
    wave_x = first_a.astype(f32) + jnp.repeat(jnp.arange(a_local, dtype=f32), KY)
    wave_y = jnp.tile(jnp.arange(KY, dtype=f32) - KC, a_local)
    wave_xy = jnp.stack([wave_x, wave_y])

    def coefficient(in_ref, f, table_ref):
        stacked = jnp.concatenate([in_ref[f, r] for r in range(rows)], axis=0)
        return dot(table_ref[...], stacked) * scale_inv

    def emit(out_ref, f, real, imag, table_ref):
        both = jnp.concatenate([real, imag], axis=0).astype(bf16)
        made = dot(table_ref[...], both).astype(bf16)
        for r in range(rows):
            out_ref[f, r] = made[r * 2 * planes : (r + 1) * 2 * planes]

    def waves(wave_ref):
        wx, wy = wave_ref[0:1, :], wave_ref[1:2, :]
        m = lax.broadcasted_iota(jnp.int32, (modes_z, cut), 0) - half_z
        wz = m.astype(f32) * (NX / total_z)
        return wx, wy, wz, wx * wx + wy * wy + wz * wz

    def lines_spec(count):
        return pl.BlockSpec((count, rows, 2 * planes, cut), lambda i: (0, 0, 0, i))

    def coeff_spec(count):
        return pl.BlockSpec((count, 2 * modes_z, cut), lambda i: (0, 0, i))

    def lines_shape(count):
        return jax.ShapeDtypeStruct((count, rows, 2 * planes, lanes), bf16)

    def coeff_shape(count):
        return jax.ShapeDtypeStruct((count, 2 * modes_z, lanes), f32)

    wave_spec = pl.BlockSpec((2, cut), lambda i: (0, i))

    def derive(in_ref, wave_ref, f_ref, i_ref, coeff_ref, out_ref):
        wx, wy, wz, k2 = waves(wave_ref)
        cs = [coefficient(in_ref, j, f_ref) for j in range(5)]
        for j in range(5):
            coeff_ref[j] = cs[j]
        re, im = [c[:modes_z] for c in cs], [c[modes_z:] for c in cs]
        emit(out_ref, 0, -(wx * im[0]), wx * re[0], i_ref)
        emit(out_ref, 1, -(wy * im[0]), wy * re[0], i_ref)
        emit(out_ref, 2, -(wz * im[0]), wz * re[0], i_ref)
        emit(out_ref, 3, -k2 * re[0], -k2 * im[0], i_ref)
        w = [wx, wy, wz]
        for j in range(3):
            p, q = (j + 1) % 3, (j + 2) % 3
            real = -(w[p] * im[1 + q] - w[q] * im[1 + p])
            emit(out_ref, 4 + j, real, w[p] * re[1 + q] - w[q] * re[1 + p], i_ref)

    def solve(in_ref, old_ref, wave_ref, f_ref, i_ref, out_ref):
        wx, wy, wz, k2 = waves(wave_ref)
        mean_mode = (wx == 0) & (wy == 0) & (wz == 0)
        stable = 1.0 / time_step + mobility * stabilizer * k2
        below = stable + mobility * epsilon * epsilon * k2 * k2
        viscous = 1.0 / time_step + k2 / reynolds
        largest = jnp.maximum(k2, 1.0)
        w = [wx, wy, wz]
        added = [coefficient(in_ref, j, f_ref) for j in range(4)]
        made = [[], [], [], []]
        for p in range(2):
            at = slice(p * modes_z, (p + 1) * modes_z)
            kept = jnp.where(mean_mode, 0.0, added[0][at])
            made[0].append((stable * old_ref[0, at] - kept - mobility * k2 * old_ref[4, at]) / below)
            free = [(old_ref[1 + j, at] / time_step + added[1 + j][at]) / viscous for j in range(3)]
            normal = (wx * free[0] + wy * free[1] + wz * free[2]) / largest
            for j in range(3):
                made[1 + j].append(free[j] - w[j] * normal)
        for j in range(4):
            emit(out_ref, j, made[j][0], made[j][1], i_ref)

    tail = [wave_spec, whole(tz_f), whole(tz_i)]
    last = (wave_xy, tz_f, tz_i)
    first_lines = first_to_spectral()
    coeffs, derived = call(
        derive, (steps,), [lines_spec(5)] + tail,
        [coeff_spec(5), lines_spec(7)], [coeff_shape(5), lines_shape(7)], COST, 1 << 20,
    )(first_lines, *last)
    fields = derived_to_physical(derived)
    gradient, vortex = fields[0:3], fields[4:7]
    advect, _, potential = phase_terms(phase, velocity, gradient, fields[3])
    forcing = momentum(velocity, vortex, gradient, potential)
    products = jnp.concatenate([advect[None], forcing], axis=0)
    product_lines = products_to_spectral(products)
    solved = call(
        solve, (steps,), [lines_spec(4), coeff_spec(5)] + tail,
        lines_spec(4), lines_shape(4), COST, 1 << 20,
    )(product_lines, coeffs, *last)
    solved_lines = solved_to_lines(solved)
    return (x_inverse(solved_lines, 0, 1)[0], x_inverse(solved_lines, 1, 3))


def solution(mesh):
    cols, rows = mesh.shape["col"], mesh.shape["row"]

    def on_device(phase, velocity):
        rows_y, planes = phase.shape[0], phase.shape[1]
        kx_local = KC // cols
        aligned = planes % 8 == 0 and kx_local % (8 * rows // math.gcd(8, rows)) == 0
        if aligned and (rows_y * planes) % 128 == 0:
            return fast_device((cols, rows, rows_y, planes), phase, velocity)
        return plain_device(phase, velocity)

    return jax.shard_map(
        on_device,
        mesh=mesh,
        in_specs=(P("col", "row", None), P(None, "col", "row", None)),
        out_specs=(P("col", "row", None), P(None, "col", "row", None)),
        check_vma=False,
    )
```
